32 devices in a mesh: tok: 2 (over x), vocab: 16 (over z, y, core).
Axes of the slice: x: 2, y: 2, z: 4, core: 2. Of those that a mesh axis runs over, the one named last changes fastest.
Arguments:
- hidden: bfloat16 [1536, 4096], P('tok', 'vocab'), as said below
- weight: bfloat16 [4096, 16384], P('tok', 'vocab'), may hold values from -0.09375 to 0.09375
- targets: int32 [1536], P('tok'), may hold values from 0 to 16383
- domains: int32 [1536], P('tok'), may hold values from 0 to 63
- seq_len: int32 [12], P('tok'), may hold values from 1 to 128
Outputs:
- token_loss: float32 [1536], P(('tok', 'vocab'))
- domain_mean: float32 [64], replicated
The draws below stay inside these ranges and needn't reach their ends.
Inputs may be any that keep to these rules, and one draw needn't show every extreme that they name: hidden states of the eval window.
All inputs are finite; a program needn't handle non-finite values.
Results may differ from the reference program's by a relative error of at most 0.0003.
Values may be sent and summed in bfloat16 or wider, within the bound.
A program may use at most 64 MiB of HBM per device.

```python
import math
import jax
import jax.numpy as jnp
import numpy as np
from jax import lax

D = 4096
VOCAB = 16384
TOK_DEV = 768
SEQ_LEN = 128
DOMAINS = 64
TOKENS = 1536
SEQS = 12


def draw_hidden(key, part):
    values = jax.random.normal(key, (TOKENS, D), jnp.float32) * 3.0
    return values.astype(jnp.bfloat16)


def set_ends(values, rng, low, top_value):
    index_at = [jax.random.randint(jax.random.fold_in(rng, axis), (), 0, length) for axis, length in enumerate(values.shape)]
    longest = values.shape.index(max(values.shape))
    next_to = index_at[:longest] + [(index_at[longest] + 1) % values.shape[longest]] + index_at[longest + 1:]
    return values.at[tuple(index_at)].set(low).at[tuple(next_to)].set(top_value)


def levels(own_key, extent, cuts, least, high):
    def one(position, shards_of):
        steps = jax.random.uniform(jax.random.fold_in(jax.random.fold_in(own_key, 6), position), (shards_of,), jnp.float32, least / len(cuts), high / len(cuts))
        return jnp.repeat(jnp.exp(steps), extent[position] // shards_of).reshape((-1,) + (1,) * (len(extent) - position - 1))

    loudness = one(*cuts[0])
    for cut in cuts[1:]:
        loudness = loudness * one(*cut)
    return loudness


def cumulative_ranks(number_of, lean):
    portions = [(1 << 20) // math.isqrt(rank ** lean) + 1 for rank in range(1, number_of + 1)]
    deviation = 1 + sum(portions) // (1 << 30)
    return np.cumsum(np.array([max(1, weight // deviation) for weight in portions]))


def ranked_ids(stream_key, shape, count, skew):
    table = cumulative_ranks(count, skew)
    ticket = jax.random.randint(jax.random.fold_in(stream_key, 1), shape, 0, int(table[count - 1]))
    standing = jnp.searchsorted(jnp.asarray(table, jnp.int32), ticket, side="right")
    return jax.random.permutation(jax.random.fold_in(stream_key, 2), count)[standing].astype(jnp.int32)


def noise(key, dims, spread, limit, shards=(), kind=jnp.bfloat16):
    result = spread * jax.random.normal(key, dims, jnp.float32)
    if shards:
        result = result * levels(key, dims, shards, -0.22, 0.18)
    return jnp.clip(result, -limit, limit).astype(kind)


def setup_inputs(seed: int = 0) -> dict:
    seeds = jax.random.split(jax.random.key(seed), 6)
    return {
        "hidden": draw_hidden(jax.random.fold_in(seeds[5], 71), 0),
        "weight": noise(seeds[1], (D, VOCAB), D ** -0.5, 0.09375, ((0, 2), (1, 16))),
        "targets": set_ends(ranked_ids(seeds[2], (TOKENS,), VOCAB, 2), jax.random.fold_in(seeds[2], 3), 0, VOCAB - 1).astype(jnp.int32),
        "domains": set_ends(jax.random.randint(seeds[3], (TOKENS,), 0, DOMAINS), jax.random.fold_in(seeds[3], 1), 0, DOMAINS - 1).astype(jnp.int32),
        "seq_len": set_ends(jax.random.randint(seeds[4], (SEQS,), 1, SEQ_LEN + 1), jax.random.fold_in(seeds[4], 1), 1, SEQ_LEN).astype(jnp.int32),
    }


def block_stats(pair):
    rows, wanted = pair
    logits = jnp.dot(rows, WEIGHT_HOLDER[0], preferred_element_type=jnp.float32)
    row_top = jnp.max(logits, axis=1)
    row_total = jnp.sum(jnp.exp(logits - row_top[:, None]), axis=1)
    picked = jnp.take_along_axis(logits, wanted[:, None].astype(jnp.int32), axis=1)[:, 0]
    return row_top, row_total, picked


WEIGHT_HOLDER = []


def reference(hidden, weight, targets, domains, seq_len):
    blocks = TOKENS // TOK_DEV

    def block_fn(pair):
        rows, wanted = pair
        logits = jnp.dot(rows, weight, preferred_element_type=jnp.float32)
        row_top = jnp.max(logits, axis=1)
        row_total = jnp.sum(jnp.exp(logits - row_top[:, None]), axis=1)
        picked = jnp.take_along_axis(logits, wanted[:, None].astype(jnp.int32), axis=1)[:, 0]
        return row_top, row_total, picked

    row_top, row_total, picked = lax.map(block_fn, (hidden.reshape(blocks, TOK_DEV, D), targets.reshape(blocks, TOK_DEV)))
    row_top = row_top.reshape(TOKENS)
    row_total = row_total.reshape(TOKENS)
    picked = picked.reshape(TOKENS)
    positions = jnp.arange(TOKENS, dtype=jnp.int32)
    lengths = seq_len[positions // SEQ_LEN]
    valid_mask = ((positions % SEQ_LEN) < lengths).astype(jnp.float32)
    token_loss = (jnp.log(row_total) + row_top - picked) * valid_mask
    onehot = (domains[:, None] == jnp.arange(DOMAINS, dtype=jnp.int32)[None, :]).astype(jnp.float32)
    domain_sum = jnp.dot(token_loss, onehot, precision=lax.Precision.HIGHEST)
    domain_count = jnp.dot(valid_mask, onehot, precision=lax.Precision.HIGHEST)
    domain_mean = domain_sum / jnp.maximum(domain_count, 1.0)
    return token_loss, domain_mean
```

```python
import functools

import jax
import jax.numpy as jnp
from jax import lax
from jax.experimental import pallas as pl
from jax.experimental.pallas import tpu as pltpu
from jax.sharding import PartitionSpec as P

SEQ_LEN = 128
DOMAINS = 64
LANES = 128
TILE = 8
GATHER_LIMIT = 24 << 20
MESH = pl.DeviceIdType.MESH


def body(hidden, weight, targets, domains, seq_len):
    features = lax.all_gather(hidden, "vocab", axis=1, tiled=True)
    tok_rows = features.shape[0]
    columns = weight.shape[1]
    logits = jnp.dot(
        features,
        lax.all_gather(weight, "tok", axis=0, tiled=True),
        preferred_element_type=jnp.float32,
    )
    first_col = lax.axis_index("vocab") * columns
    column_ids = first_col + lax.broadcasted_iota(jnp.int32, (tok_rows, columns), 1)
    picked_loc = jnp.sum(jnp.where(column_ids == targets[:, None], logits, 0.0), axis=1)
    top_loc = jnp.max(logits, axis=1)
    groups = lax.axis_size("vocab")
    share_len = tok_rows // groups
    sum_loc = jnp.sum(jnp.exp(logits - top_loc[:, None]), axis=1)
    gathered = [
        lax.all_to_all(
            part.reshape(groups, share_len), "vocab", split_axis=0, concat_axis=0, tiled=True
        )
        for part in (top_loc, sum_loc, picked_loc)
    ]
    row_top = jnp.max(gathered[0], axis=0)
    row_total = jnp.sum(gathered[1] * jnp.exp(gathered[0] - row_top[None, :]), axis=0)
    picked = jnp.sum(gathered[2], axis=0)
    loss_raw = jnp.log(row_total) + row_top - picked
    valid_mask, domain_share = token_share(domains, seq_len, share_len)
    token_loss = loss_raw * valid_mask
    onehot = (
        domain_share[:, None] == lax.broadcasted_iota(jnp.int32, (share_len, DOMAINS), 1)
    ).astype(jnp.float32)
    domain_sum = jnp.dot(token_loss, onehot, precision=lax.Precision.HIGHEST)
    domain_count = jnp.dot(valid_mask, onehot, precision=lax.Precision.HIGHEST)
    domain_sum, domain_count = lax.psum((domain_sum, domain_count), ("tok", "vocab"))
    domain_mean = domain_sum / jnp.maximum(domain_count, 1.0)
    return (token_loss, domain_mean)


def token_share(domains, seq_len, share_len):
    share_start = lax.axis_index("vocab") * share_len
    positions = share_start + lax.iota(jnp.int32, share_len)
    seq_ids = positions // SEQ_LEN
    seq_count = seq_len.shape[0]
    lengths = jnp.sum(
        jnp.where(
            seq_ids[:, None] == lax.broadcasted_iota(jnp.int32, (share_len, seq_count), 1),
            seq_len[None, :],
            0,
        ),
        axis=1,
    )
    valid_mask = (positions % SEQ_LEN < lengths).astype(jnp.float32)
    return valid_mask, lax.dynamic_slice_in_dim(domains, share_start, share_len)


@functools.lru_cache(None)
def plan(depth):
    queues = {}
    have = [dict() for _ in range(depth)]
    for z in range(depth):
        have[z][(0, 0, z)] = 0.0
        have[z][(1, 0, z)] = 1.0
    pending = [(have[z][s], z, s) for z in range(depth) for s in have[z]]
    free = {}
    sends = [dict() for _ in range(depth)]

    def push(now, z, link, shard):
        start = max(now, free.get((z, link), 0.0))
        free[(z, link)] = start + 1.0
        to, item = {
            "y": (z, (shard[0], 1, shard[2])),
            "up": (z + 1, shard),
            "down": (z - 1, shard),
        }[link]
        have[to][item] = start + 1.0
        pending.append((start + 1.0, to, item))
        sends[z].setdefault(shard, []).append(link)

    while pending:
        pending.sort()
        now, z, shard = pending.pop(0)
        sends[z].setdefault(shard, [])
        if shard[1]:
            continue
        if z < depth - 1 and shard[2] <= z:
            push(now, z, "up", shard)
        if z > 0 and shard[2] >= z:
            push(now, z, "down", shard)
        if not (shard[0] == 0 and shard[2] == (z ^ 1)):
            push(now, z, "y", shard)
    for z in range(depth):
        link = "up" if z % 2 == 0 else "down"
        start = max(have[z][(0, 1, z)], free[(z, link)])
        have[z ^ 1][(0, 1, z)] = start + 1.0
    order = []
    for z in range(depth):
        link = "up" if z % 2 == 0 else "down"
        events = sorted((time, shard) for shard, time in have[z].items())
        after = max(
            [i for i, (_, s) in enumerate(events) if link in sends[z].get(s, ())]
            + [i for i, (_, s) in enumerate(events) if s == (0, 1, z)]
        )
        rows = []
        for i, (time, shard) in enumerate(events):
            links = list(sends[z].get(shard, []))
            rows.append((time, shard, links + (["far"] if i == after else [])))
        order.append(rows)
    return order


@functools.lru_cache(None)
def program(depth):
    order = plan(depth)
    pieces = 4 * depth // 2
    weight_order, products = {}, {}
    for t in range(2):
        for z in range(depth):
            arrival = {s: time for time, s, _ in order[z]}
            remote = [zz for zz in range(depth) if zz // (depth // 2) != t]
            remote.sort(key=lambda zz: (abs(zz - z), zz))
            chunks = [(zz, dy, dc) for zz in remote for dy in range(2) for dc in range(2)]
            weight_order[(t, z)] = chunks
            at = {ch: 1.0 + (i + 1) * 16.0 / 3 / pieces for i, ch in enumerate(chunks)}
            ready = []
            for zz in range(depth):
                for dy in range(2):
                    for dc in range(2):
                        time = max(arrival[(0, dy, zz)], arrival[(1, dy, zz)]) + 0.15 * dc
                        ready.append((max(time, at.get((zz, dy, dc), 0.0)), (zz, dy, dc)))
            products[(t, z)] = sorted(ready)
    keys = sorted(products)
    count = len(order[0])
    steps = [
        (sum(order[z][i][0] for z in range(depth)) / depth, 0, i) for i in range(1, count)
    ]
    steps += [
        (sum(products[k][i][0] for k in keys) / len(keys) + 0.2, 1, i)
        for i in range(len(products[keys[0]]))
    ]
    steps.sort()
    arrived = {z: {order[z][0][1]} for z in range(depth)}
    sequence, waiting = [], []

    def ready_now(i):
        return all(
            products[k][i][1][2] == 1
            or {(0,) + products[k][i][1][1::-1], (1,) + products[k][i][1][1::-1]}
            <= arrived[k[1]]
            for k in keys
        )

    for _, kind, i in steps:
        if kind == 0:
            sequence.append((0, i))
            for z in range(depth):
                arrived[z].add(order[z][i][1])
        else:
            waiting.append(i)
        while waiting and ready_now(waiting[0]):
            sequence.append((1, waiting.pop(0)))
    assert not waiting
    return order, weight_order, products, sequence


def kernel(
    depth, hid, weight, tgt, dom, mask, loss_out, mean_out,
    held, wts, acc, tgt_all, tgt_col, stat, stat_in, part, part_in,
    own_sem, held_sem, wts_sem, send_sem, wsend_sem, tgt_sem,
    s1_send, s1_recv, s2_send, s2_recv,
):
    order, weight_order, products, sequence = program(depth)
    t, v = lax.axis_index("tok"), lax.axis_index("vocab")
    vocab = 4 * depth
    devices = 2 * vocab
    me = t * vocab + v
    z, y, c = v // 4, (v // 2) % 2, v % 2
    tok_rows, kb = hid.shape
    cols = wts.shape[2]
    locals_ = vocab // 2
    share = tok_rows // vocab

    def sel(values, index):
        if all(a == values[0] for a in values):
            return values[0]
        out = jnp.int32(values[0])
        for i, a in enumerate(values[1:], 1):
            out = jnp.where(index == i, jnp.int32(a), out)
        return out

    key = t * depth + z

    own = pltpu.make_async_copy(hid, held.at[t, v], own_sem.at[0])
    own.start()
    own_tgt = pltpu.make_async_copy(tgt, tgt_all.at[t], own_sem.at[1])
    own_tgt.start()

    def mine(r):
        return pltpu.make_async_copy(
            weight.at[pl.ds(r * kb, kb), pl.ds(pl.multiple_of(t * cols, LANES), cols)],
            wts.at[t * locals_ + r],
            wts_sem.at[t * locals_ + r],
        )

    for r in range(locals_):
        mine(r).start()

    barrier = pltpu.get_barrier_semaphore()

    def greet(k, carry):
        other = (me + k) % devices
        pl.semaphore_signal(
            barrier, inc=1, device_id=(other // vocab, other % vocab), device_id_type=MESH
        )
        return carry

    lax.fori_loop(1, devices, greet, 0)
    own.wait()
    own_tgt.wait()
    pl.semaphore_wait(barrier, devices - 1)

    where = {
        "x": lambda: (1 - t, v),
        "y": lambda: (t, v + 2 - 4 * y),
        "up": lambda: (t, v + 4),
        "down": lambda: (t, v - 4),
        "far": lambda: (t, v + 4 - 8 * (z % 2)),
        "pair": lambda: (t, v + 1 - 2 * c),
    }
    lanes_of = {"x": 0, "y": 1, "up": 2, "down": 3, "far": 4, "pair": 5}
    sent = []

    def send(tt, vv, link, step, places):
        copy = pltpu.make_async_remote_copy(
            src_ref=held.at[tt, vv],
            dst_ref=held.at[tt, vv],
            send_sem=send_sem.at[step, lanes_of[link]],
            recv_sem=held_sem.at[tt, vv],
            device_id=where[link](),
            device_id_type=MESH,
        )
        guarded(places, copy.start)
        sent.append((places, copy))

    def guarded(places, act):
        if len(places) == depth:
            act()
            return
        hit = z == places[0]
        for p in places[1:]:
            hit = jnp.logical_or(hit, z == p)
        pl.when(hit)(act)

    def fan_out(step):
        tt = (t + sel([order[p][step][1][0] for p in range(depth)], z)) % 2
        yy = (y + sel([order[p][step][1][1] for p in range(depth)], z)) % 2
        zz = sel([order[p][step][1][2] for p in range(depth)], z)
        vv = zz * 4 + yy * 2 + c
        if step:
            pltpu.make_async_copy(hid, held.at[tt, vv], held_sem.at[tt, vv]).wait()
        if not step:
            send(tt, vv, "x", 0, list(range(depth)))
        for link in ("up", "down", "y"):
            places = [p for p in range(depth) if link in order[p][step][2]]
            if places:
                send(tt, vv, link, step, places)
        send(tt, vv, "pair", step, list(range(depth)))
        places = [p for p in range(depth) if "far" in order[p][step][2]]
        if places:
            send(t, z * 4 + (1 - y) * 2 + c, "far", step, places)

    fan_out(0)
    tgt_copy = pltpu.make_async_remote_copy(
        src_ref=tgt_all.at[t], dst_ref=tgt_all.at[t],
        send_sem=tgt_sem.at[0], recv_sem=tgt_sem.at[1],
        device_id=where["x"](), device_id_type=MESH,
    )
    tgt_copy.start()

    wsent = []
    for i in range(locals_):
        chunk = [weight_order[(1 - k // depth, k % depth)][i] for k in range(2 * depth)]
        zz = sel([ch[0] for ch in chunk], key)
        yy = (y + sel([ch[1] for ch in chunk], key)) % 2
        cc = (c + sel([ch[2] for ch in chunk], key)) % 2
        vv = zz * 4 + yy * 2 + cc
        row = pl.multiple_of((vv - t * locals_) * kb, kb)
        copy = pltpu.make_async_remote_copy(
            src_ref=weight.at[pl.ds(row, kb), pl.ds(pl.multiple_of((1 - t) * cols, LANES), cols)],
            dst_ref=wts.at[vv],
            send_sem=wsend_sem.at[i],
            recv_sem=wts_sem.at[vv],
            device_id=where["x"](),
            device_id_type=MESH,
        )
        copy.start()
        wsent.append(copy)

    tgt_copy.wait()

    def spread(i, carry):
        for h in range(2):
            row = tgt_all[h, pl.ds(i, 1), :].astype(jnp.float32)
            tgt_col[pl.ds(pl.multiple_of(h * tok_rows + i * LANES, LANES), LANES), :] = jnp.transpose(
                jnp.broadcast_to(row, (LANES, LANES))
            )
        return carry

    lax.fori_loop(0, tok_rows // LANES, spread, 0)

    def product(i, first):
        chunk = [products[(k // depth, k % depth)][i][1] for k in range(2 * depth)]
        zz = sel([ch[0] for ch in chunk], key)
        yy = (y + sel([ch[1] for ch in chunk], key)) % 2
        dc = sel([ch[2] for ch in chunk], key)
        vv = zz * 4 + yy * 2 + (c + dc) % 2

        def wait_pair():
            for h in range(2):
                pltpu.make_async_copy(hid, held.at[h, vv], held_sem.at[h, vv]).wait()

        if isinstance(dc, int):
            if dc:
                wait_pair()
        else:
            pl.when(dc == 1)(wait_pair)
        pltpu.make_async_copy(wts.at[vv], wts.at[vv], wts_sem.at[vv]).wait()
        step_rows = 256 if tok_rows % 256 == 0 else LANES

        def tile(r, carry):
            for h in range(2):
                at = pl.ds(pl.multiple_of(r * step_rows, step_rows), step_rows)
                to = pl.ds(pl.multiple_of(h * tok_rows + r * step_rows, step_rows), step_rows)
                got = jnp.dot(held[h, vv, at, :], wts[vv], preferred_element_type=jnp.float32)
                if first:
                    acc[to, :] = got
                else:
                    acc[to, :] += got
            return carry

        lax.fori_loop(0, tok_rows // step_rows, tile, 0)

    first = True
    for kind, i in sequence:
        if kind == 0:
            fan_out(i)
        else:
            product(i, first)
            first = False

    first_col = (v * 2 + t) * cols
    lane = lax.broadcasted_iota(jnp.int32, (share, LANES), 1)
    col = lax.broadcasted_iota(jnp.int32, (share, cols), 1)

    def finish(w, carry):
        rows = pl.ds(pl.multiple_of(w * share, share), share)
        got = acc[rows, :]
        wanted = tgt_col[rows, 0:1].astype(jnp.int32) - first_col
        top = jnp.max(got, axis=1, keepdims=True)
        total = jnp.sum(jnp.exp(got - top), axis=1, keepdims=True)
        picked = jnp.sum(jnp.where(col == wanted, got, 0.0), axis=1, keepdims=True)
        both = jnp.where(lane == 0, top, jnp.where(lane == 1, total, picked))
        both = jnp.concatenate([both, jnp.zeros((LANES - share, LANES), jnp.float32)], axis=0)
        stat[w] = jnp.transpose(both)[:TILE, :]
        return carry

    lax.fori_loop(0, devices, finish, 0)

    def exchange(src_at, dst, send, recv):
        def copy(k):
            other = (me + k) % devices
            return pltpu.make_async_remote_copy(
                src_ref=src_at(other), dst_ref=dst.at[me],
                send_sem=send.at[other], recv_sem=recv.at[me],
                device_id=(other // vocab, other % vocab), device_id_type=MESH,
            )

        def go(k, carry):
            copy(k).start()
            return carry

        def done(k, carry):
            other = (me + k) % devices
            copy(k).wait_send()
            pltpu.make_async_copy(dst.at[other], dst.at[other], recv.at[other]).wait()
            return carry

        lax.fori_loop(1, devices, go, 0)
        lax.fori_loop(1, devices, done, 0)

    exchange(lambda other: stat.at[other], stat_in, s1_send, s1_recv)
    stat_in[me] = stat[me]

    every = stat_in[...]
    tops, totals, picks = every[:, 0, :], every[:, 1, :], every[:, 2, :]
    row_top = jnp.max(tops, axis=0, keepdims=True)
    row_total = jnp.sum(totals * jnp.exp(tops - row_top), axis=0, keepdims=True)
    picked = jnp.sum(picks, axis=0, keepdims=True)
    inside = lax.broadcasted_iota(jnp.int32, (1, LANES), 1) < share
    valid = mask[...]
    raw = jnp.where(inside, jnp.log(jnp.where(inside, row_total, 1.0)) + row_top - picked, 0.0)
    loss = raw * valid
    loss_out[...] = loss

    def column(row):
        return jnp.transpose(jnp.broadcast_to(row, (LANES, LANES)))

    hot = dom[...] == lax.broadcasted_iota(jnp.int32, (LANES, LANES), 1)
    part[0:1, :] = jnp.sum(jnp.where(hot, column(loss), 0.0), axis=0, keepdims=True)
    part[1:2, :] = jnp.sum(jnp.where(hot, column(valid), 0.0), axis=0, keepdims=True)
    part[2:TILE, :] = jnp.zeros((TILE - 2, LANES), jnp.float32)
    exchange(lambda other: part, part_in, s2_send, s2_recv)
    part_in[me] = part[...]
    sums = jnp.sum(part_in[...], axis=0)
    mean_out[...] = sums[0:1, :] / jnp.maximum(sums[1:2, :], 1.0)

    for places, copy in sent:
        guarded(places, copy.wait_send)
    for copy in wsent:
        copy.wait_send()


def kernel_body(hidden, weight, targets, domains, seq_len):
    vocab = lax.axis_size("vocab")
    depth = vocab // 4
    devices = 2 * vocab
    tok_rows, kb = hidden.shape
    columns = weight.shape[1] // 2
    share = tok_rows // vocab
    valid, domain_share = token_share(domains, seq_len, share)
    valid = jnp.pad(valid, (0, LANES - share)).reshape(1, LANES)
    dom = jnp.broadcast_to(
        jnp.pad(domain_share, (0, LANES - share), constant_values=-1)[:, None], (LANES, LANES)
    )
    tgt = targets.reshape(tok_rows // LANES, LANES)
    steps = 4 * depth
    anywhere = pl.BlockSpec(memory_space=pl.ANY)
    vmem = pl.BlockSpec(memory_space=pltpu.VMEM)
    dma = pltpu.SemaphoreType.DMA
    loss, mean = pl.pallas_call(
        functools.partial(kernel, depth),
        out_shape=[jax.ShapeDtypeStruct((1, LANES), jnp.float32)] * 2,
        in_specs=[anywhere, anywhere, vmem, vmem, vmem],
        out_specs=[vmem, vmem],
        scratch_shapes=[
            pltpu.VMEM((2, vocab, tok_rows, kb), jnp.bfloat16),
            pltpu.VMEM((vocab, kb, columns), jnp.bfloat16),
            pltpu.VMEM((2 * tok_rows, columns), jnp.float32),
            pltpu.VMEM((2,) + tgt.shape, jnp.int32),
            pltpu.VMEM((2 * tok_rows, LANES), jnp.float32),
            pltpu.VMEM((devices, TILE, LANES), jnp.float32),
            pltpu.VMEM((devices, TILE, LANES), jnp.float32),
            pltpu.VMEM((TILE, LANES), jnp.float32),
            pltpu.VMEM((devices, TILE, LANES), jnp.float32),
            dma((2,)),
            dma((2, vocab)),
            dma((vocab,)),
            dma((steps, 6)),
            dma((vocab // 2,)),
            dma((2,)),
            dma((devices,)),
            dma((devices,)),
            dma((devices,)),
            dma((devices,)),
        ],
        compiler_params=pltpu.CompilerParams(
            collective_id=0, has_side_effects=True, vmem_limit_bytes=40 << 20
        ),
        cost_estimate=pl.CostEstimate(
            flops=4 * tok_rows * kb * vocab * columns, bytes_accessed=16 << 20, transcendentals=0
        ),
    )(hidden, weight, tgt, dom, valid)
    return loss[0, :share], mean[0, :DOMAINS]


def solution(mesh):
    tok, vocab = mesh.shape["tok"], mesh.shape["vocab"]

    def step(hidden, weight, targets, domains, seq_len):
        tok_rows = hidden.shape[0]
        fits = (
            tok == 2
            and vocab % 8 == 0
            and tok * tok_rows * weight.shape[0] * tok * 2 <= GATHER_LIMIT
            and tok_rows % (LANES * 2) == 0
            and tok_rows % (vocab * TILE) == 0
            and tok_rows // vocab <= LANES
            and weight.shape[1] % (2 * LANES) == 0
            and hidden.shape[1] % LANES == 0
        )
        chosen = kernel_body if fits else body
        return chosen(hidden, weight, targets, domains, seq_len)

    in_specs = (P("tok", "vocab"), P("tok", "vocab"), P("tok"), P("tok"), P("tok"))
    out_specs = (P(("tok", "vocab")), P())
    return jax.shard_map(step, mesh=mesh, in_specs=in_specs, out_specs=out_specs, check_vma=False)
```

```python
import functools

import jax
import jax.numpy as jnp
from jax import lax
from jax.experimental import pallas as pl
from jax.experimental.pallas import tpu as pltpu
from jax.sharding import PartitionSpec as P

SEQ_LEN = 128
DOMAINS = 64
LANES = 128
TILE = 8
GATHER_LIMIT = 24 << 20
PARTS = 2
STATS = 4
MESH = pl.DeviceIdType.MESH


def body(hidden, weight, targets, domains, seq_len):
    features = lax.all_gather(hidden, "vocab", axis=1, tiled=True)
    tok_rows = features.shape[0]
    columns = weight.shape[1]
    logits = jnp.dot(
        features,
        lax.all_gather(weight, "tok", axis=0, tiled=True),
        preferred_element_type=jnp.float32,
    )
    first_col = lax.axis_index("vocab") * columns
    column_ids = first_col + lax.broadcasted_iota(jnp.int32, (tok_rows, columns), 1)
    picked_loc = jnp.sum(jnp.where(column_ids == targets[:, None], logits, 0.0), axis=1)
    top_loc = jnp.max(logits, axis=1)
    groups = lax.axis_size("vocab")
    share_len = tok_rows // groups
    sum_loc = jnp.sum(jnp.exp(logits - top_loc[:, None]), axis=1)
    gathered = [
        lax.all_to_all(
            part.reshape(groups, share_len), "vocab", split_axis=0, concat_axis=0, tiled=True
        )
        for part in (top_loc, sum_loc, picked_loc)
    ]
    row_top = jnp.max(gathered[0], axis=0)
    row_total = jnp.sum(gathered[1] * jnp.exp(gathered[0] - row_top[None, :]), axis=0)
    picked = jnp.sum(gathered[2], axis=0)
    loss_raw = jnp.log(row_total) + row_top - picked
    valid_mask, domain_share = token_share(domains, seq_len, share_len)
    token_loss = loss_raw * valid_mask
    onehot = (
        domain_share[:, None] == lax.broadcasted_iota(jnp.int32, (share_len, DOMAINS), 1)
    ).astype(jnp.float32)
    domain_sum = jnp.dot(token_loss, onehot, precision=lax.Precision.HIGHEST)
    domain_count = jnp.dot(valid_mask, onehot, precision=lax.Precision.HIGHEST)
    domain_sum, domain_count = lax.psum((domain_sum, domain_count), ("tok", "vocab"))
    domain_mean = domain_sum / jnp.maximum(domain_count, 1.0)
    return (token_loss, domain_mean)


def token_share(domains, seq_len, share_len):
    share_start = lax.axis_index("vocab") * share_len
    positions = share_start + lax.iota(jnp.int32, share_len)
    seq_ids = positions // SEQ_LEN
    seq_count = seq_len.shape[0]
    lengths = jnp.sum(
        jnp.where(
            seq_ids[:, None] == lax.broadcasted_iota(jnp.int32, (share_len, seq_count), 1),
            seq_len[None, :],
            0,
        ),
        axis=1,
    )
    valid_mask = (positions % SEQ_LEN < lengths).astype(jnp.float32)
    return valid_mask, lax.dynamic_slice_in_dim(domains, share_start, share_len)


@functools.lru_cache(None)
def plan(depth):
    queues = {}
    have = [dict() for _ in range(depth)]
    for z in range(depth):
        for h in range(PARTS):
            have[z][(0, 0, z, h)] = 0.0
            have[z][(1, 0, z, h)] = (h + 1.0) / PARTS
    pending = [(have[z][s], z, s) for z in range(depth) for s in have[z]]
    free = {}
    sends = [dict() for _ in range(depth)]

    def push(now, z, link, shard):
        start = max(now, free.get((z, link), 0.0))
        free[(z, link)] = start + 1.0 / PARTS
        to, item = {
            "y": (z, (shard[0], 1) + shard[2:]),
            "up": (z + 1, shard),
            "down": (z - 1, shard),
        }[link]
        have[to][item] = start + 1.0 / PARTS
        pending.append((start + 1.0 / PARTS, to, item))
        sends[z].setdefault(shard, []).append(link)

    while pending:
        pending.sort()
        now, z, shard = pending.pop(0)
        sends[z].setdefault(shard, [])
        if shard[1]:
            continue
        if z < depth - 1 and shard[2] <= z:
            push(now, z, "up", shard)
        if z > 0 and shard[2] >= z:
            push(now, z, "down", shard)
        if not (shard[0] == 0 and shard[2] == (z ^ 1)):
            push(now, z, "y", shard)
    for z in range(depth):
        link = "up" if z % 2 == 0 else "down"
        for h in range(PARTS):
            start = max(have[z][(0, 1, z, h)], free[(z, link)])
            free[(z, link)] = start + 1.0 / PARTS
            have[z ^ 1][(0, 1, z, h)] = start + 1.0 / PARTS
    order = []
    for z in range(depth):
        link = "up" if z % 2 == 0 else "down"
        events = sorted((time, shard) for shard, time in have[z].items())
        after = max(
            [i for i, (_, s) in enumerate(events) if link in sends[z].get(s, ())]
            + [i for i, (_, s) in enumerate(events) if s[:3] == (0, 1, z)]
        )
        rows = []
        for i, (time, shard) in enumerate(events):
            links = list(sends[z].get(shard, []))
            rows.append((time, shard, links + (["far"] if i == after else [])))
        order.append(rows)
    return order


@functools.lru_cache(None)
def program(depth):
    order = plan(depth)
    pieces = 4 * depth // 2
    weight_order, products = {}, {}
    for t in range(2):
        for z in range(depth):
            arrival = {s: time for time, s, _ in order[z]}
            remote = [zz for zz in range(depth) if zz // (depth // 2) != t]
            remote.sort(key=lambda zz: (abs(zz - z), zz))
            chunks = [(zz, dy, dc) for zz in remote for dy in range(2) for dc in range(2)]
            weight_order[(t, z)] = chunks
            at = {ch: 1.0 + (i + 1) * 16.0 / 3 / pieces for i, ch in enumerate(chunks)}
            ready = []
            for zz in range(depth):
                for dy in range(2):
                    for dc in range(2):
                        time = max(a for s, a in arrival.items() if s[1:3] == (dy, zz)) + 0.15 * dc
                        ready.append((max(time, at.get((zz, dy, dc), 0.0)), (zz, dy, dc)))
            products[(t, z)] = sorted(ready)
    keys = sorted(products)
    count = len(order[0])
    steps = [
        (sum(order[z][i][0] for z in range(depth)) / depth, 0, i) for i in range(PARTS, count)
    ]
    steps += [
        (sum(products[k][i][0] for k in keys) / len(keys) + 0.2, 1, i)
        for i in range(len(products[keys[0]]))
    ]
    steps.sort()
    arrived = {z: {order[z][i][1] for i in range(PARTS)} for z in range(depth)}
    sequence, waiting = [], []

    def ready_now(i):
        return all(
            products[k][i][1][2] == 1
            or sum(s[1:3] == products[k][i][1][1::-1] for s in arrived[k[1]]) == 2 * PARTS
            for k in keys
        )

    for _, kind, i in steps:
        if kind == 0:
            sequence.append((0, i))
            for z in range(depth):
                arrived[z].add(order[z][i][1])
        else:
            waiting.append(i)
        while waiting and ready_now(waiting[0]):
            sequence.append((1, waiting.pop(0)))
    assert not waiting
    return order, weight_order, products, sequence


def kernel(
    depth, hid, weight, tgt, dom, seq, loss_out, mean_out,
    held, wts, turned, acc, tgt_all, dom_all, stat, stat_in, part, part_in,
    own_sem, held_sem, wts_sem, send_sem, wsend_sem, tgt_sem,
    s1_send, s1_recv, s2_send, s2_recv,
):
    order, weight_order, products, sequence = program(depth)
    t, v = lax.axis_index("tok"), lax.axis_index("vocab")
    vocab = 4 * depth
    devices = 2 * vocab
    me = t * vocab + v
    z, y, c = v // 4, (v // 2) % 2, v % 2
    tok_rows, kb = hid.shape
    cols = wts.shape[2]
    locals_ = vocab // 2
    share = tok_rows // vocab

    def sel(values, index):
        if all(a == values[0] for a in values):
            return values[0]
        out = jnp.int32(values[0])
        for i, a in enumerate(values[1:], 1):
            out = jnp.where(index == i, jnp.int32(a), out)
        return out

    key = t * depth + z

    rows_of = tok_rows // PARTS
    owns = [
        pltpu.make_async_copy(hid.at[pl.ds(h * rows_of, rows_of)], held.at[t, v, h], own_sem.at[2 + h])
        for h in range(PARTS)
    ]
    for own in owns:
        own.start()
    own_dom = pltpu.make_async_copy(dom, dom_all, own_sem.at[0])
    own_dom.start()
    own_tgt = pltpu.make_async_copy(tgt, tgt_all.at[t], own_sem.at[1])
    own_tgt.start()

    def mine(r):
        return pltpu.make_async_copy(
            weight.at[pl.ds(r * kb, kb), pl.ds(pl.multiple_of(t * cols, LANES), cols)],
            wts.at[t * locals_ + r],
            wts_sem.at[t * locals_ + r],
        )

    for r in range(locals_):
        mine(r).start()

    barrier = pltpu.get_barrier_semaphore()

    def greet(k, carry):
        other = (me + k) % devices
        pl.semaphore_signal(
            barrier, inc=1, device_id=(other // vocab, other % vocab), device_id_type=MESH
        )
        return carry

    lax.fori_loop(1, devices, greet, 0)
    for own in owns:
        own.wait()
    own_tgt.wait()
    own_dom.wait()
    pl.semaphore_wait(barrier, devices - 1)

    where = {
        "x": lambda: (1 - t, v),
        "y": lambda: (t, v + 2 - 4 * y),
        "up": lambda: (t, v + 4),
        "down": lambda: (t, v - 4),
        "far": lambda: (t, v + 4 - 8 * (z % 2)),
        "pair": lambda: (t, v + 1 - 2 * c),
    }
    lanes_of = {"x": 0, "y": 1, "up": 2, "down": 3, "far": 4, "pair": 5}
    sent = []

    def send(tt, vv, h, link, step, places, lane=None):
        copy = pltpu.make_async_remote_copy(
            src_ref=held.at[tt, vv, h],
            dst_ref=held.at[tt, vv, h],
            send_sem=send_sem.at[step, lanes_of[link] if lane is None else lane],
            recv_sem=held_sem.at[tt, vv, h],
            device_id=where[link](),
            device_id_type=MESH,
        )
        guarded(places, copy.start)
        sent.append((places, copy))

    def guarded(places, act):
        if len(places) == depth:
            act()
            return
        hit = z == places[0]
        for p in places[1:]:
            hit = jnp.logical_or(hit, z == p)
        pl.when(hit)(act)

    def fan_out(step):
        tt = (t + sel([order[p][step][1][0] for p in range(depth)], z)) % 2
        yy = (y + sel([order[p][step][1][1] for p in range(depth)], z)) % 2
        zz = sel([order[p][step][1][2] for p in range(depth)], z)
        vv = zz * 4 + yy * 2 + c
        h = sel([order[p][step][1][3] for p in range(depth)], z)
        if step >= PARTS:
            landed(tt, vv, h)
        else:
            send(tt, vv, h, "x", step, list(range(depth)))
        for link in ("up", "down", "y"):
            places = [p for p in range(depth) if link in order[p][step][2]]
            if places:
                send(tt, vv, h, link, step, places)
        send(tt, vv, h, "pair", step, list(range(depth)))
        places = [p for p in range(depth) if "far" in order[p][step][2]]
        if places:
            for part_ in range(PARTS):
                send(t, z * 4 + (1 - y) * 2 + c, part_, "far", step, places, 6 + part_)

    def landed(tt, vv, h):
        pltpu.make_async_copy(held.at[tt, vv, h], held.at[tt, vv, h], held_sem.at[tt, vv, h]).wait()

    for step in range(PARTS):
        fan_out(step)
    tgt_copy = pltpu.make_async_remote_copy(
        src_ref=tgt_all.at[t], dst_ref=tgt_all.at[t],
        send_sem=tgt_sem.at[0], recv_sem=tgt_sem.at[1],
        device_id=where["x"](), device_id_type=MESH,
    )
    tgt_copy.start()

    wsent = []
    for i in range(locals_):
        chunk = [weight_order[(1 - k // depth, k % depth)][i] for k in range(2 * depth)]
        zz = sel([ch[0] for ch in chunk], key)
        yy = (y + sel([ch[1] for ch in chunk], key)) % 2
        cc = (c + sel([ch[2] for ch in chunk], key)) % 2
        vv = zz * 4 + yy * 2 + cc
        row = pl.multiple_of((vv - t * locals_) * kb, kb)
        copy = pltpu.make_async_remote_copy(
            src_ref=weight.at[pl.ds(row, kb), pl.ds(pl.multiple_of((1 - t) * cols, LANES), cols)],
            dst_ref=wts.at[vv],
            send_sem=wsend_sem.at[i],
            recv_sem=wts_sem.at[vv],
            device_id=where["x"](),
            device_id_type=MESH,
        )
        copy.start()
        wsent.append(copy)

    tgt_copy.wait()

    def product(i, first):
        chunk = [products[(k // depth, k % depth)][i][1] for k in range(2 * depth)]
        zz = sel([ch[0] for ch in chunk], key)
        yy = (y + sel([ch[1] for ch in chunk], key)) % 2
        dc = sel([ch[2] for ch in chunk], key)
        vv = zz * 4 + yy * 2 + (c + dc) % 2

        def wait_pair():
            for h in range(2):
                for part_ in range(PARTS):
                    landed(h, vv, part_)

        if isinstance(dc, int):
            if dc:
                wait_pair()
        else:
            pl.when(dc == 1)(wait_pair)
        pltpu.make_async_copy(wts.at[vv], wts.at[vv], wts_sem.at[vv]).wait()
        turned[...] = jnp.transpose(wts[vv])

        def tile(r, carry):
            to = pl.ds(pl.multiple_of(r * rows_of, LANES), rows_of)
            got = lax.dot_general(
                turned[...], held[r // PARTS, vv, r % PARTS], (((1,), (1,)), ((), ())),
                preferred_element_type=jnp.float32,
            )
            if first:
                acc[:, to] = got
            else:
                acc[:, to] += got
            return carry

        lax.fori_loop(0, 2 * PARTS, tile, 0)

    first = True
    for kind, i in sequence:
        if kind == 0:
            fan_out(i)
        else:
            product(i, first)
            first = False

    first_col = (v * 2 + t) * cols
    tiles = tok_rows // LANES
    col = lax.broadcasted_iota(jnp.int32, (cols, LANES), 0)

    def finish(b, carry):
        got = acc[:, pl.ds(pl.multiple_of(b * LANES, LANES), LANES)]
        wanted = tgt_all[b // tiles, pl.ds(b % tiles, 1), :] - first_col
        top = jnp.max(got, axis=0, keepdims=True)
        total = jnp.sum(jnp.exp(got - top), axis=0, keepdims=True)
        picked = jnp.sum(jnp.where(col == wanted, got, 0.0), axis=0, keepdims=True)
        stat[b] = jnp.concatenate([top, total, picked, picked], axis=0)
        return carry

    lax.fori_loop(0, 2 * tiles, finish, 0)

    def first_tile(vv):
        return jnp.minimum(vv * share // LANES, tiles - 2)

    def exchange(src_at, dst, send, recv):
        def copy(k):
            other = (me + k) % devices
            return pltpu.make_async_remote_copy(
                src_ref=src_at(other), dst_ref=dst.at[me],
                send_sem=send.at[other], recv_sem=recv.at[me],
                device_id=(other // vocab, other % vocab), device_id_type=MESH,
            )

        def go(k, carry):
            copy(k).start()
            return carry

        def done(k, carry):
            other = (me + k) % devices
            copy(k).wait_send()
            pltpu.make_async_copy(dst.at[other], dst.at[other], recv.at[other]).wait()
            return carry

        lax.fori_loop(1, devices, go, 0)
        lax.fori_loop(1, devices, done, 0)

    def window(other):
        return pl.ds(other // vocab * tiles + first_tile(other % vocab), 2)

    exchange(lambda other: stat.at[window(other)], stat_in, s1_send, s1_recv)
    stat_in[me] = stat[window(me)]

    def column(row):
        return jnp.transpose(jnp.broadcast_to(row, (LANES, LANES)))

    tile0 = first_tile(v)
    lane = lax.broadcasted_iota(jnp.int32, (1, LANES), 1)
    classes = lax.broadcasted_iota(jnp.int32, (LANES, LANES), 1).astype(jnp.float32)
    sums, counts = jnp.zeros((1, LANES), jnp.float32), jnp.zeros((1, LANES), jnp.float32)
    for j in range(2):
        tops, totals, picks = (stat_in[:, j, row, :] for row in range(3))
        row_top = jnp.max(tops, axis=0, keepdims=True)
        row_total = jnp.sum(totals * jnp.exp(tops - row_top), axis=0, keepdims=True)
        picked = jnp.sum(picks, axis=0, keepdims=True)
        position = (tile0 + j) * LANES + lane
        inside = jnp.logical_and(position >= v * share, position < (v + 1) * share)
        valid = jnp.where(inside, (lane < seq[tile0 + j]).astype(jnp.float32), 0.0)
        loss = (jnp.log(row_total) + row_top - picked) * valid
        loss_out[j : j + 1, :] = loss
        hot = column(dom_all[pl.ds(tile0 + j, 1), :].astype(jnp.float32)) == classes
        sums += jnp.sum(jnp.where(hot, column(loss), 0.0), axis=0, keepdims=True)
        counts += jnp.sum(jnp.where(hot, column(valid), 0.0), axis=0, keepdims=True)
    part[...] = jnp.concatenate([sums, counts], axis=0)
    exchange(lambda other: part, part_in, s2_send, s2_recv)
    part_in[me] = part[...]
    sums = jnp.sum(part_in[...], axis=0)
    mean_out[...] = sums[0:1, :] / jnp.maximum(sums[1:2, :], 1.0)

    for places, copy in sent:
        guarded(places, copy.wait_send)
    for copy in wsent:
        copy.wait_send()


def kernel_body(hidden, weight, targets, domains, seq_len):
    vocab = lax.axis_size("vocab")
    depth = vocab // 4
    devices = 2 * vocab
    tok_rows, kb = hidden.shape
    columns = weight.shape[1] // 2
    share = tok_rows // vocab
    tiles = tok_rows // LANES
    anywhere = pl.BlockSpec(memory_space=pl.ANY)
    vmem = pl.BlockSpec(memory_space=pltpu.VMEM)
    dma = pltpu.SemaphoreType.DMA
    loss, mean = pl.pallas_call(
        functools.partial(kernel, depth),
        out_shape=[
            jax.ShapeDtypeStruct((2, LANES), jnp.float32),
            jax.ShapeDtypeStruct((1, LANES), jnp.float32),
        ],
        in_specs=[anywhere] * 4 + [pl.BlockSpec(memory_space=pltpu.SMEM)],
        out_specs=[vmem, vmem],
        scratch_shapes=[
            pltpu.VMEM((2, vocab, PARTS, tok_rows // PARTS, kb), jnp.bfloat16),
            pltpu.VMEM((vocab, kb, columns), jnp.bfloat16),
            pltpu.VMEM((columns, kb), jnp.bfloat16),
            pltpu.VMEM((columns, 2 * tok_rows), jnp.float32),
            pltpu.VMEM((2, tiles, LANES), jnp.int32),
            pltpu.VMEM((tiles, LANES), jnp.int32),
            pltpu.VMEM((2 * tiles, STATS, LANES), jnp.float32),
            pltpu.VMEM((devices, 2, STATS, LANES), jnp.float32),
            pltpu.VMEM((2, LANES), jnp.float32),
            pltpu.VMEM((devices, 2, LANES), jnp.float32),
            dma((2 + PARTS,)),
            dma((2, vocab, PARTS)),
            dma((vocab,)),
            dma((4 * depth * PARTS, 6 + PARTS)),
            dma((vocab // 2,)),
            dma((2,)),
            dma((devices,)),
            dma((devices,)),
            dma((devices,)),
            dma((devices,)),
        ],
        compiler_params=pltpu.CompilerParams(
            collective_id=0, has_side_effects=True, vmem_limit_bytes=60 * 1024 * 1024
        ),
        cost_estimate=pl.CostEstimate(
            flops=4 * tok_rows * kb * vocab * columns, bytes_accessed=16 << 20, transcendentals=0
        ),
    )(
        hidden, weight, targets.reshape(tiles, LANES), domains.reshape(tiles, LANES), seq_len
    )
    start = lax.axis_index("vocab") * share
    start = start - jnp.minimum(start // LANES, tiles - 2) * LANES
    return lax.dynamic_slice_in_dim(loss.reshape(2 * LANES), start, share), mean[0, :DOMAINS]


def solution(mesh):
    tok, vocab = mesh.shape["tok"], mesh.shape["vocab"]

    def step(hidden, weight, targets, domains, seq_len):
        tok_rows = hidden.shape[0]
        fits = (
            tok == 2
            and vocab % 8 == 0
            and tok * tok_rows * weight.shape[0] * tok * 2 <= GATHER_LIMIT
            and tok_rows % (LANES * PARTS) == 0
            and SEQ_LEN == LANES
            and tok_rows % (vocab * TILE) == 0
            and tok_rows // vocab <= LANES
            and weight.shape[1] % (2 * LANES) == 0
            and hidden.shape[1] % LANES == 0
        )
        chosen = kernel_body if fits else body
        return chosen(hidden, weight, targets, domains, seq_len)

    in_specs = (P("tok", "vocab"), P("tok", "vocab"), P("tok"), P("tok"), P("tok"))
    out_specs = (P(("tok", "vocab")), P())
    return jax.shard_map(step, mesh=mesh, in_specs=in_specs, out_specs=out_specs, check_vma=False)
```

```python
import functools

import jax
import jax.numpy as jnp
from jax import lax
from jax.experimental import pallas as pl
from jax.experimental.pallas import tpu as pltpu
from jax.sharding import PartitionSpec as P

SEQ_LEN = 128
DOMAINS = 64
LANES = 128
TILE = 8
GATHER_LIMIT = 24 << 20
PARTS = 1
STATS = 4
MESH = pl.DeviceIdType.MESH


def body(hidden, weight, targets, domains, seq_len):
    features = lax.all_gather(hidden, "vocab", axis=1, tiled=True)
    tok_rows = features.shape[0]
    columns = weight.shape[1]
    logits = jnp.dot(
        features,
        lax.all_gather(weight, "tok", axis=0, tiled=True),
        preferred_element_type=jnp.float32,
    )
    first_col = lax.axis_index("vocab") * columns
    column_ids = first_col + lax.broadcasted_iota(jnp.int32, (tok_rows, columns), 1)
    picked_loc = jnp.sum(jnp.where(column_ids == targets[:, None], logits, 0.0), axis=1)
    top_loc = jnp.max(logits, axis=1)
    groups = lax.axis_size("vocab")
    share_len = tok_rows // groups
    sum_loc = jnp.sum(jnp.exp(logits - top_loc[:, None]), axis=1)
    gathered = [
        lax.all_to_all(
            part.reshape(groups, share_len), "vocab", split_axis=0, concat_axis=0, tiled=True
        )
        for part in (top_loc, sum_loc, picked_loc)
    ]
    row_top = jnp.max(gathered[0], axis=0)
    row_total = jnp.sum(gathered[1] * jnp.exp(gathered[0] - row_top[None, :]), axis=0)
    picked = jnp.sum(gathered[2], axis=0)
    loss_raw = jnp.log(row_total) + row_top - picked
    valid_mask, domain_share = token_share(domains, seq_len, share_len)
    token_loss = loss_raw * valid_mask
    onehot = (
        domain_share[:, None] == lax.broadcasted_iota(jnp.int32, (share_len, DOMAINS), 1)
    ).astype(jnp.float32)
    domain_sum = jnp.dot(token_loss, onehot, precision=lax.Precision.HIGHEST)
    domain_count = jnp.dot(valid_mask, onehot, precision=lax.Precision.HIGHEST)
    domain_sum, domain_count = lax.psum((domain_sum, domain_count), ("tok", "vocab"))
    domain_mean = domain_sum / jnp.maximum(domain_count, 1.0)
    return (token_loss, domain_mean)


def token_share(domains, seq_len, share_len):
    share_start = lax.axis_index("vocab") * share_len
    positions = share_start + lax.iota(jnp.int32, share_len)
    seq_ids = positions // SEQ_LEN
    seq_count = seq_len.shape[0]
    lengths = jnp.sum(
        jnp.where(
            seq_ids[:, None] == lax.broadcasted_iota(jnp.int32, (share_len, seq_count), 1),
            seq_len[None, :],
            0,
        ),
        axis=1,
    )
    valid_mask = (positions % SEQ_LEN < lengths).astype(jnp.float32)
    return valid_mask, lax.dynamic_slice_in_dim(domains, share_start, share_len)


@functools.lru_cache(None)
def plan(depth):
    queues = {}
    have = [dict() for _ in range(depth)]
    for z in range(depth):
        for h in range(PARTS):
            have[z][(0, 0, z, h)] = 0.0
            have[z][(1, 0, z, h)] = (h + 1.0) / PARTS
    pending = [(have[z][s], z, s) for z in range(depth) for s in have[z]]
    free = {}
    sends = [dict() for _ in range(depth)]

    def push(now, z, link, shard):
        start = max(now, free.get((z, link), 0.0))
        free[(z, link)] = start + 1.0 / PARTS
        to, item = {
            "y": (z, (shard[0], 1) + shard[2:]),
            "up": (z + 1, shard),
            "down": (z - 1, shard),
        }[link]
        have[to][item] = start + 1.0 / PARTS
        pending.append((start + 1.0 / PARTS, to, item))
        sends[z].setdefault(shard, []).append(link)

    while pending:
        pending.sort()
        now, z, shard = pending.pop(0)
        sends[z].setdefault(shard, [])
        if shard[1]:
            continue
        if z < depth - 1 and shard[2] <= z:
            push(now, z, "up", shard)
        if z > 0 and shard[2] >= z:
            push(now, z, "down", shard)
        if not (shard[0] == 0 and shard[2] == (z ^ 1)):
            push(now, z, "y", shard)
    for z in range(depth):
        link = "up" if z % 2 == 0 else "down"
        for h in range(PARTS):
            start = max(have[z][(0, 1, z, h)], free[(z, link)])
            free[(z, link)] = start + 1.0 / PARTS
            have[z ^ 1][(0, 1, z, h)] = start + 1.0 / PARTS
    order = []
    for z in range(depth):
        link = "up" if z % 2 == 0 else "down"
        events = sorted((time, shard) for shard, time in have[z].items())
        after = max(
            [i for i, (_, s) in enumerate(events) if link in sends[z].get(s, ())]
            + [i for i, (_, s) in enumerate(events) if s[:3] == (0, 1, z)]
        )
        rows = []
        for i, (time, shard) in enumerate(events):
            links = list(sends[z].get(shard, []))
            rows.append((time, shard, links + (["far"] if i == after else [])))
        order.append(rows)
    return order


@functools.lru_cache(None)
def program(depth):
    order = plan(depth)
    pieces = 4 * depth // 2
    weight_order, products = {}, {}
    for t in range(2):
        for z in range(depth):
            arrival = {s: time for time, s, _ in order[z]}
            remote = [zz for zz in range(depth) if zz // (depth // 2) != t]
            remote.sort(key=lambda zz: (abs(zz - z), zz))
            chunks = [(zz, dy, dc) for zz in remote for dy in range(2) for dc in range(2)]
            weight_order[(t, z)] = chunks
            at = {ch: 1.0 + (i + 1) * 16.0 / 3 / pieces for i, ch in enumerate(chunks)}
            ready = []
            for zz in range(depth):
                for dy in range(2):
                    for dc in range(2):
                        time = max(a for s, a in arrival.items() if s[1:3] == (dy, zz)) + 0.15 * dc
                        ready.append((max(time, at.get((zz, dy, dc), 0.0)), (zz, dy, dc)))
            products[(t, z)] = sorted(ready)
    keys = sorted(products)
    count = len(order[0])
    steps = [
        (sum(order[z][i][0] for z in range(depth)) / depth, 0, i) for i in range(PARTS, count)
    ]
    steps += [
        (sum(products[k][i][0] for k in keys) / len(keys) + 0.2, 1, i)
        for i in range(len(products[keys[0]]))
    ]
    steps.sort()
    arrived = {z: {order[z][i][1] for i in range(PARTS)} for z in range(depth)}
    sequence, waiting = [], []

    def ready_now(i):
        return all(
            products[k][i][1][2] == 1
            or sum(s[1:3] == products[k][i][1][1::-1] for s in arrived[k[1]]) == 2 * PARTS
            for k in keys
        )

    for _, kind, i in steps:
        if kind == 0:
            sequence.append((0, i))
            for z in range(depth):
                arrived[z].add(order[z][i][1])
        else:
            waiting.append(i)
        while waiting and ready_now(waiting[0]):
            sequence.append((1, waiting.pop(0)))
    assert not waiting
    return order, weight_order, products, sequence


def count_sends(depth):
    order = plan(depth)
    total = PARTS + len(order[0])
    for step in range(len(order[0])):
        links = {link for rows in order for link in rows[step][2]}
        total += len(links - {"far"}) + PARTS * ("far" in links)
    return total


def kernel(
    depth, hid, weight, tgt, dom, seq, loss_out, mean_out,
    held, wts, turned, acc, tgt_all, dom_all, stat, stat_in, part, part_in,
    own_sem, held_sem, wts_sem, send_sem, wsend_sem, tgt_sem,
    s1_send, s1_recv, s2_send, s2_recv,
):
    order, weight_order, products, sequence = program(depth)
    t, v = lax.axis_index("tok"), lax.axis_index("vocab")
    vocab = 4 * depth
    devices = 2 * vocab
    me = t * vocab + v
    z, y, c = v // 4, (v // 2) % 2, v % 2
    tok_rows, kb = hid.shape
    cols = wts.shape[2]
    locals_ = vocab // 2
    share = tok_rows // vocab

    def sel(values, index):
        if all(a == values[0] for a in values):
            return values[0]
        out = jnp.int32(values[0])
        for i, a in enumerate(values[1:], 1):
            out = jnp.where(index == i, jnp.int32(a), out)
        return out

    key = t * depth + z

    rows_of = tok_rows // PARTS
    owns = [
        pltpu.make_async_copy(hid.at[pl.ds(h * rows_of, rows_of)], held.at[t, v, h], own_sem.at[2 + h])
        for h in range(PARTS)
    ]
    for own in owns:
        own.start()
    own_dom = pltpu.make_async_copy(dom, dom_all, own_sem.at[0])
    own_dom.start()
    own_tgt = pltpu.make_async_copy(tgt, tgt_all.at[t], own_sem.at[1])
    own_tgt.start()

    def mine(r):
        return pltpu.make_async_copy(
            weight.at[pl.ds(r * kb, kb), pl.ds(pl.multiple_of(t * cols, LANES), cols)],
            wts.at[t * locals_ + r],
            wts_sem.at[t * locals_ + r],
        )

    for r in range(locals_):
        mine(r).start()

    barrier = pltpu.get_barrier_semaphore()

    def greet(k, carry):
        other = (me + k) % devices
        pl.semaphore_signal(
            barrier, inc=1, device_id=(other // vocab, other % vocab), device_id_type=MESH
        )
        return carry

    lax.fori_loop(1, devices, greet, 0)
    for own in owns:
        own.wait()
    own_tgt.wait()
    own_dom.wait()
    pl.semaphore_wait(barrier, devices - 1)

    where = {
        "x": lambda: (1 - t, v),
        "y": lambda: (t, v + 2 - 4 * y),
        "up": lambda: (t, v + 4),
        "down": lambda: (t, v - 4),
        "far": lambda: (t, v + 4 - 8 * (z % 2)),
        "pair": lambda: (t, v + 1 - 2 * c),
    }
    sent = []

    def send(tt, vv, h, link, places):
        copy = pltpu.make_async_remote_copy(
            src_ref=held.at[tt, vv, h],
            dst_ref=held.at[tt, vv, h],
            send_sem=send_sem.at[len(sent)],
            recv_sem=held_sem.at[tt, vv, h],
            device_id=where[link](),
            device_id_type=MESH,
        )
        guarded(places, copy.start)
        sent.append((places, copy))

    def guarded(places, act):
        if len(places) == depth:
            act()
            return
        hit = z == places[0]
        for p in places[1:]:
            hit = jnp.logical_or(hit, z == p)
        pl.when(hit)(act)

    def fan_out(step):
        tt = (t + sel([order[p][step][1][0] for p in range(depth)], z)) % 2
        yy = (y + sel([order[p][step][1][1] for p in range(depth)], z)) % 2
        zz = sel([order[p][step][1][2] for p in range(depth)], z)
        vv = zz * 4 + yy * 2 + c
        h = sel([order[p][step][1][3] for p in range(depth)], z)
        if step >= PARTS:
            landed(tt, vv, h)
        else:
            send(tt, vv, h, "x", list(range(depth)))
        for link in ("up", "down", "y"):
            places = [p for p in range(depth) if link in order[p][step][2]]
            if places:
                send(tt, vv, h, link, places)
        send(tt, vv, h, "pair", list(range(depth)))
        places = [p for p in range(depth) if "far" in order[p][step][2]]
        if places:
            for part_ in range(PARTS):
                send(t, z * 4 + (1 - y) * 2 + c, part_, "far", places)

    def landed(tt, vv, h):
        pltpu.make_async_copy(held.at[tt, vv, h], held.at[tt, vv, h], held_sem.at[tt, vv, h]).wait()

    for step in range(PARTS):
        fan_out(step)
    tgt_copy = pltpu.make_async_remote_copy(
        src_ref=tgt_all.at[t], dst_ref=tgt_all.at[t],
        send_sem=tgt_sem.at[0], recv_sem=tgt_sem.at[1],
        device_id=where["x"](), device_id_type=MESH,
    )
    tgt_copy.start()

    wsent = []
    for i in range(locals_):
        chunk = [weight_order[(1 - k // depth, k % depth)][i] for k in range(2 * depth)]
        zz = sel([ch[0] for ch in chunk], key)
        yy = (y + sel([ch[1] for ch in chunk], key)) % 2
        cc = (c + sel([ch[2] for ch in chunk], key)) % 2
        vv = zz * 4 + yy * 2 + cc
        row = pl.multiple_of((vv - t * locals_) * kb, kb)
        copy = pltpu.make_async_remote_copy(
            src_ref=weight.at[pl.ds(row, kb), pl.ds(pl.multiple_of((1 - t) * cols, LANES), cols)],
            dst_ref=wts.at[vv],
            send_sem=wsend_sem.at[i],
            recv_sem=wts_sem.at[vv],
            device_id=where["x"](),
            device_id_type=MESH,
        )
        copy.start()
        wsent.append(copy)

    tgt_copy.wait()

    def product(i, first):
        chunk = [products[(k // depth, k % depth)][i][1] for k in range(2 * depth)]
        zz = sel([ch[0] for ch in chunk], key)
        yy = (y + sel([ch[1] for ch in chunk], key)) % 2
        dc = sel([ch[2] for ch in chunk], key)
        vv = zz * 4 + yy * 2 + (c + dc) % 2

        def wait_pair():
            for h in range(2):
                for part_ in range(PARTS):
                    landed(h, vv, part_)

        if isinstance(dc, int):
            if dc:
                wait_pair()
        else:
            pl.when(dc == 1)(wait_pair)
        pltpu.make_async_copy(wts.at[vv], wts.at[vv], wts_sem.at[vv]).wait()
        turned[...] = jnp.transpose(wts[vv])

        def tile(r, carry):
            to = pl.ds(pl.multiple_of(r * rows_of, LANES), rows_of)
            got = lax.dot_general(
                turned[...], held[r // PARTS, vv, r % PARTS], (((1,), (1,)), ((), ())),
                preferred_element_type=jnp.float32,
            )
            if first:
                acc[:, to] = got
            else:
                acc[:, to] += got
            return carry

        lax.fori_loop(0, 2 * PARTS, tile, 0)

    first = True
    for kind, i in sequence:
        if kind == 0:
            fan_out(i)
        else:
            product(i, first)
            first = False

    first_col = (v * 2 + t) * cols
    tiles = tok_rows // LANES
    col = lax.broadcasted_iota(jnp.int32, (cols, LANES), 0)

    def finish(b, carry):
        got = acc[:, pl.ds(pl.multiple_of(b * LANES, LANES), LANES)]
        wanted = tgt_all[b // tiles, pl.ds(b % tiles, 1), :] - first_col
        top = jnp.max(got, axis=0, keepdims=True)
        total = jnp.sum(jnp.exp(got - top), axis=0, keepdims=True)
        picked = jnp.sum(jnp.where(col == wanted, got, 0.0), axis=0, keepdims=True)
        stat[b] = jnp.concatenate([top, total, picked, picked], axis=0)
        return carry

    lax.fori_loop(0, 2 * tiles, finish, 0)

    def first_tile(vv):
        return jnp.minimum(vv * share // LANES, tiles - 2)

    def exchange(src_at, dst, send, recv):
        def copy(k):
            other = (me + k) % devices
            return pltpu.make_async_remote_copy(
                src_ref=src_at(other), dst_ref=dst.at[me],
                send_sem=send.at[0], recv_sem=recv.at[0],
                device_id=(other // vocab, other % vocab), device_id_type=MESH,
            )

        def go(k, carry):
            copy(k).start()
            return carry

        lax.fori_loop(1, devices, go, 0)
        others = dst.at[pl.ds(0, devices - 1)]
        pltpu.make_async_copy(others, others, send.at[0]).wait()
        pltpu.make_async_copy(others, others, recv.at[0]).wait()

    def window(other):
        return pl.ds(other // vocab * tiles + first_tile(other % vocab), 2)

    exchange(lambda other: stat.at[window(other)], stat_in, s1_send, s1_recv)
    stat_in[me] = stat[window(me)]

    def column(row):
        return jnp.transpose(jnp.broadcast_to(row, (LANES, LANES)))

    tile0 = first_tile(v)
    lane = lax.broadcasted_iota(jnp.int32, (1, LANES), 1)
    classes = lax.broadcasted_iota(jnp.int32, (LANES, LANES), 1).astype(jnp.float32)
    sums, counts = jnp.zeros((1, LANES), jnp.float32), jnp.zeros((1, LANES), jnp.float32)
    for j in range(2):
        tops, totals, picks = (stat_in[:, j, row, :] for row in range(3))
        row_top = jnp.max(tops, axis=0, keepdims=True)
        row_total = jnp.sum(totals * jnp.exp(tops - row_top), axis=0, keepdims=True)
        picked = jnp.sum(picks, axis=0, keepdims=True)
        position = (tile0 + j) * LANES + lane
        inside = jnp.logical_and(position >= v * share, position < (v + 1) * share)
        valid = jnp.where(inside, (lane < seq[tile0 + j]).astype(jnp.float32), 0.0)
        loss = (jnp.log(row_total) + row_top - picked) * valid
        loss_out[j : j + 1, :] = loss
        hot = column(dom_all[pl.ds(tile0 + j, 1), :].astype(jnp.float32)) == classes
        sums += jnp.sum(jnp.where(hot, column(loss), 0.0), axis=0, keepdims=True)
        counts += jnp.sum(jnp.where(hot, column(valid), 0.0), axis=0, keepdims=True)
    part[...] = jnp.concatenate([sums, counts], axis=0)
    exchange(lambda other: part, part_in, s2_send, s2_recv)
    part_in[me] = part[...]
    sums = jnp.sum(part_in[...], axis=0)
    mean_out[...] = sums[0:1, :] / jnp.maximum(sums[1:2, :], 1.0)

    for places, copy in sent:
        guarded(places, copy.wait_send)
    for copy in wsent:
        copy.wait_send()


def kernel_body(hidden, weight, targets, domains, seq_len):
    vocab = lax.axis_size("vocab")
    depth = vocab // 4
    devices = 2 * vocab
    tok_rows, kb = hidden.shape
    columns = weight.shape[1] // 2
    share = tok_rows // vocab
    tiles = tok_rows // LANES
    anywhere = pl.BlockSpec(memory_space=pl.ANY)
    vmem = pl.BlockSpec(memory_space=pltpu.VMEM)
    dma = pltpu.SemaphoreType.DMA
    loss, mean = pl.pallas_call(
        functools.partial(kernel, depth),
        out_shape=[
            jax.ShapeDtypeStruct((2, LANES), jnp.float32),
            jax.ShapeDtypeStruct((1, LANES), jnp.float32),
        ],
        in_specs=[anywhere] * 4 + [pl.BlockSpec(memory_space=pltpu.SMEM)],
        out_specs=[vmem, vmem],
        scratch_shapes=[
            pltpu.VMEM((2, vocab, PARTS, tok_rows // PARTS, kb), jnp.bfloat16),
            pltpu.VMEM((vocab, kb, columns), jnp.bfloat16),
            pltpu.VMEM((columns, kb), jnp.bfloat16),
            pltpu.VMEM((columns, 2 * tok_rows), jnp.float32),
            pltpu.VMEM((2, tiles, LANES), jnp.int32),
            pltpu.VMEM((tiles, LANES), jnp.int32),
            pltpu.VMEM((2 * tiles, STATS, LANES), jnp.float32),
            pltpu.VMEM((devices, 2, STATS, LANES), jnp.float32),
            pltpu.VMEM((2, LANES), jnp.float32),
            pltpu.VMEM((devices, 2, LANES), jnp.float32),
            dma((2 + PARTS,)),
            dma((2, vocab, PARTS)),
            dma((vocab,)),
            dma((count_sends(depth),)),
            dma((vocab // 2,)),
            dma((2,)),
            dma((1,)),
            dma((1,)),
            dma((1,)),
            dma((1,)),
        ],
        compiler_params=pltpu.CompilerParams(
            collective_id=0, has_side_effects=True, vmem_limit_bytes=60 * 1024 * 1024
        ),
        cost_estimate=pl.CostEstimate(
            flops=4 * tok_rows * kb * vocab * columns, bytes_accessed=16 << 20, transcendentals=0
        ),
    )(
        hidden, weight, targets.reshape(tiles, LANES), domains.reshape(tiles, LANES), seq_len
    )
    start = lax.axis_index("vocab") * share
    start = start - jnp.minimum(start // LANES, tiles - 2) * LANES
    return lax.dynamic_slice_in_dim(loss.reshape(2 * LANES), start, share), mean[0, :DOMAINS]


def solution(mesh):
    tok, vocab = mesh.shape["tok"], mesh.shape["vocab"]

    def step(hidden, weight, targets, domains, seq_len):
        tok_rows = hidden.shape[0]
        fits = (
            tok == 2
            and vocab % 8 == 0
            and tok * tok_rows * weight.shape[0] * tok * 2 <= GATHER_LIMIT
            and tok_rows % (LANES * PARTS) == 0
            and SEQ_LEN == LANES
            and tok_rows % (vocab * TILE) == 0
            and tok_rows // vocab <= LANES
            and weight.shape[1] % (2 * LANES) == 0
            and hidden.shape[1] % LANES == 0
        )
        chosen = kernel_body if fits else body
        return chosen(hidden, weight, targets, domains, seq_len)

    in_specs = (P("tok", "vocab"), P("tok", "vocab"), P("tok"), P("tok"), P("tok"))
    out_specs = (P(("tok", "vocab")), P())
    return jax.shard_map(step, mesh=mesh, in_specs=in_specs, out_specs=out_specs, check_vma=False)
```
